768 devices in a mesh: section: 192 (over x, y_lo, z), tensor: 4 (over y_hi, core).
Axes of the slice: x: 4, y: 8 (y_hi: 2, y_lo: 4; y = y_hi * 4 + y_lo), z: 12, core: 2. Of those that a mesh axis runs over, the one named last changes fastest.
Arguments:
- hidden: bfloat16 [24576, 12288], P('section', 'tensor'), may hold values from -6 to 6
- cotangent: bfloat16 [24576, 12288], P('section', 'tensor'), may hold values from -6 to 6
- encoder: bfloat16 [12288, 1536], P('tensor'), may hold values from -0.0546875 to 0.0546875
- lengths: int32 [192], P('section'), may hold values from 64 to 128
Outputs:
- decoded: bfloat16 [24576, 12288], P('section', 'tensor')
- hidden_gradient: bfloat16 [24576, 12288], P('section', 'tensor')
The draws below stay inside these ranges and needn't reach their ends.
All inputs are finite; a program needn't handle non-finite values.
Results may differ from the reference program's by a relative error of at most 0.0083.
Values may be sent and summed in bfloat16 or wider, within the bound.
A program may use at most 32 MiB of HBM per device.

```python
import jax
import jax.numpy as jnp
from jax import lax

MODEL_WIDTH = 12288
LATENT = 1536
TOK = 128
SECTIONS = 192
ROWS = 24576


def with_ends(drawn, rng, least, high):
    index_at = [jax.random.randint(jax.random.fold_in(rng, axis), (), 0, length) for axis, length in enumerate(drawn.shape)]
    longest = drawn.shape.index(max(drawn.shape))
    neighbour = index_at[:longest] + [(index_at[longest] + 1) % drawn.shape[longest]] + index_at[longest + 1:]
    return drawn.at[tuple(index_at)].set(least).at[tuple(neighbour)].set(high)


def block_levels(key, extent, pieces, least, top_value):
    gain = 1.0
    for dim, parts in pieces:
        steps = jax.random.uniform(jax.random.fold_in(jax.random.fold_in(key, 6), dim), (parts,), jnp.float32, least / len(pieces), top_value / len(pieces))
        gain = gain * jnp.repeat(jnp.exp(steps), extent[dim] // parts).reshape((-1,) + (1,) * (len(extent) - 1 - dim))
    return gain


def scatter_about(key, extent, deviation, reach, pieces=(), kind=jnp.bfloat16):
    values = deviation * jax.random.normal(key, extent, jnp.float32)
    if pieces:
        values = values * block_levels(key, extent, pieces, -0.22, 0.18)
    return jnp.clip(values, -reach, reach).astype(kind)


def setup_inputs(seed: int = 0) -> dict:
    key_list = jax.random.split(jax.random.key(seed), 5)
    hidden = scatter_about(key_list[0], (ROWS, MODEL_WIDTH), 1.0, 6.0, ((0, 192), (1, 4)))
    cotangent = scatter_about(key_list[1], (ROWS, MODEL_WIDTH), 1.0, 6.0, ((0, 192), (1, 4)))
    encoder = scatter_about(key_list[2], (MODEL_WIDTH, LATENT), MODEL_WIDTH ** -0.5, 0.0546875, ((0, 4),))
    lengths = with_ends(jax.random.randint(key_list[3], (SECTIONS,), TOK // 2, TOK + 1), jax.random.fold_in(key_list[3], 1), TOK // 2, TOK).astype(jnp.int32)
    return dict(hidden=hidden, cotangent=cotangent, encoder=encoder, lengths=lengths)


EPS = 1e-05

def reference(hidden, cotangent, encoder, lengths):
    value_entries = hidden.astype(jnp.float32)
    row_average = lax.optimization_barrier(jnp.sum(value_entries, axis=1, keepdims=True)) / MODEL_WIDTH
    meansq = lax.optimization_barrier(jnp.sum(value_entries * value_entries, axis=1, keepdims=True)) / MODEL_WIDTH
    inverse_deviation = lax.rsqrt(meansq - row_average * row_average + EPS)
    normalized_input = (value_entries - row_average) * inverse_deviation
    colsum = lax.optimization_barrier(jnp.sum(encoder.astype(jnp.float32), axis=0))[None, :]
    position = jnp.arange(TOK, dtype=jnp.int32)
    mask = (position[None, :] < lengths[:, None]).astype(jnp.float32).reshape(SECTIONS * TOK, 1)
    product = jnp.dot(hidden, encoder, preferred_element_type=jnp.float32)
    latent = (mask * inverse_deviation * (product - row_average * colsum)).astype(jnp.bfloat16)
    received = jnp.roll(latent.reshape(SECTIONS, TOK, LATENT), 1, axis=0).reshape(SECTIONS * TOK, LATENT)
    decoded = jnp.dot(received, encoder.T, preferred_element_type=jnp.float32).astype(jnp.bfloat16)
    latent_grad = jnp.dot(cotangent, encoder, preferred_element_type=jnp.float32).astype(jnp.bfloat16)
    back = jnp.roll(latent_grad.reshape(SECTIONS, TOK, LATENT), -1, axis=0).reshape(SECTIONS * TOK, LATENT)
    back = back * mask.astype(jnp.bfloat16)
    normalized_gradient = jnp.dot(back, encoder.T, preferred_element_type=jnp.float32)
    first_piece = lax.optimization_barrier(jnp.sum(normalized_gradient, axis=1, keepdims=True)) / MODEL_WIDTH
    second_piece = lax.optimization_barrier(jnp.sum(normalized_gradient * normalized_input, axis=1, keepdims=True)) / MODEL_WIDTH
    hidden_gradient = (inverse_deviation * (normalized_gradient - first_piece - normalized_input * second_piece)).astype(jnp.bfloat16)
    return (decoded, hidden_gradient)
```

```python
import functools

import jax
import jax.numpy as jnp
from jax import lax
from jax.experimental import pallas as pl
from jax.experimental.pallas import tpu as pltpu
from jax.sharding import PartitionSpec as P

MODEL_WIDTH = 12288
EPS = 1e-05
MESH = pl.DeviceIdType.MESH
F32 = jnp.float32
BF16 = jnp.bfloat16

ROWS = 128
DEPTH = 3072
BLOCK = 256
HALF = 128
PER = 3
BLOCKS = 2 * PER
SPLIT = 4
CHUNK = DEPTH // SPLIT


def column(row):
    return jnp.broadcast_to(row, (ROWS, HALF)).T


def row_of(square):
    return jnp.sum(square.T, axis=0, keepdims=True)


def kernel(
    sections,
    hidden,
    cotangent,
    encoder,
    lengths,
    decoded,
    gradient,
    x,
    enc,
    part,
    part_in,
    colsum,
    ys,
    yr,
    gs,
    ls,
    zs,
    back,
    recv,
    stat_out,
    stat_in,
    piece_out,
    piece_in,
    acc_b,
    acc_r,
    out_d,
    out_g,
    load_sem,
    part_ss,
    part_rs,
    y_ss,
    y_rs,
    stat_ss,
    stat_rs,
    shift_ss,
    shift_rs,
    gy_ss,
    gy_rs,
    gd_ss,
    gd_rs,
    gf_ss,
    gf_rs,
    piece_ss,
    piece_rs,
    out_sem,
):
    s = lax.axis_index("section")
    t = lax.axis_index("tensor")
    c = lax.rem(t, 2)
    chip = t // 2
    t_core = chip * 2 + (1 - c)
    t_far = (1 - chip) * 2 + c
    t_diag = (1 - chip) * 2 + (1 - c)
    core = {"section": s, "tensor": t_core}
    far = {"section": s, "tensor": t_far}
    diag = {"section": s, "tensor": t_diag}
    after = {"section": lax.rem(s + 1, sections), "tensor": t}
    before = {"section": lax.rem(s + sections - 1, sections), "tensor": t}
    peers = (core, far, diag)

    def remote(src, dst, ss, rs, to):
        return pltpu.make_async_remote_copy(
            src_ref=src, dst_ref=dst, send_sem=ss, recv_sem=rs, device_id=to, device_id_type=MESH
        )

    def load_encoder(p):
        b = lax.rem(PER * (1 - chip) + p, BLOCKS)
        at = pl.ds(pl.multiple_of(b * BLOCK, BLOCK), BLOCK)
        return pltpu.make_async_copy(encoder.at[:, at], enc.at[p], load_sem.at[2 + p])

    load_c = pltpu.make_async_copy(cotangent, x.at[pl.ds(0, ROWS)], load_sem.at[0])
    load_h = pltpu.make_async_copy(hidden, x.at[pl.ds(ROWS, ROWS)], load_sem.at[1])

    def send_part(p):
        return remote(part.at[p, 1 - c], part_in.at[p], part_ss.at[p], part_rs.at[p], core)

    def send_far(a, j):
        i = a * PER + j
        return remote(ys.at[i], yr.at[i], y_ss.at[i], y_rs.at[i], far)

    def send_stat(k):
        return remote(stat_out.at[k], stat_in.at[k], stat_ss.at[k], stat_rs.at[k], peers[k])

    def send_piece(k):
        return remote(piece_out, piece_in.at[k], piece_ss.at[k], piece_rs.at[k], peers[k])

    def shift(a, j):
        i = a * PER + j
        src, dst, to = ((gs, back, before), (ls, recv, after))[a]
        return remote(src.at[j], dst.at[PER + j, c], shift_ss.at[i], shift_rs.at[i], to)

    def gather_far(a, j):
        i = a * PER + j
        buf = (back, recv)[a]
        return remote(buf.at[PER + j, c], buf.at[j, c], gy_ss.at[i], gy_rs.at[i], far)

    def gather_core(a, j):
        i = a * PER + j
        buf = (back, recv)[a]
        return remote(buf.at[PER + j, c], buf.at[PER + j, c], gd_ss.at[i], gd_rs.at[i], core)

    def pass_core(a, j):
        i = a * PER + j
        buf = (back, recv)[a]
        return remote(buf.at[j, c], buf.at[j, c], gf_ss.at[i], gf_rs.at[i], core)

    def loop(body):
        def step(j, carry):
            body(j)
            return carry

        lax.fori_loop(0, PER, step, 0)

    load_h.start()
    load_c.start()
    load_encoder(0).start()
    load_encoder(1).start()
    barrier = pltpu.get_barrier_semaphore()
    for to in (core, far, diag, after, before):
        pl.semaphore_signal(barrier, inc=1, device_id=to, device_id_type=MESH)
    x[pl.ds(2 * ROWS, 16), :] = jnp.ones((16, DEPTH), BF16)

    load_h.wait()
    total = jnp.zeros((ROWS, HALF), F32)
    square = jnp.zeros((ROWS, HALF), F32)
    for i in range(DEPTH // HALF):
        v = x[ROWS : 2 * ROWS, i * HALF : (i + 1) * HALF].astype(F32)
        total = total + v
        square = square + v * v
    total = row_of(total)
    square = row_of(square)
    own_mean = total / DEPTH
    mean_here = column(own_mean)
    stat_out[...] = jnp.zeros(stat_out.shape, F32)
    for k in range(4):
        stat_out[k, 3:4, :] = total
        stat_out[k, 4:5, :] = square
    load_c.wait()

    def encode(p):
        load_encoder(p).wait()
        y = jnp.dot(x[...], enc[p], preferred_element_type=F32)
        for h in range(2):
            at = slice(h * HALF, (h + 1) * HALF)
            cs = y[2 * ROWS : 2 * ROWS + 1, at]
            part[p, h, 0:ROWS, :] = y[0:ROWS, at]
            part[p, h, ROWS : 2 * ROWS, :] = y[ROWS : 2 * ROWS, at] - mean_here * cs
            colsum[p, h] = y[2 * ROWS : 2 * ROWS + 8, at]

    def first_blocks(j):
        load_encoder(j + 2).start()
        encode(j)

    loop(first_blocks)
    load_encoder(PER + 2).start()
    pl.semaphore_wait(barrier, 5)

    def start_parts(j):
        send_part(j).start()

    loop(start_parts)

    def last_blocks(j):
        encode(PER + j)
        send_part(PER + j).start()
        send_part(j).wait_recv()
        total_here = part[j, c] + part_in[j]
        ys[j] = total_here[0:ROWS].astype(BF16)
        ys[PER + j] = total_here[ROWS : 2 * ROWS].astype(BF16)
        send_far(0, j).start()

    loop(last_blocks)

    for j in range(PER):
        stat_out[0, j : j + 1, :] = colsum[PER + j, 1 - c][0:1]
        stat_out[1, j : j + 1, :] = colsum[j, c][0:1]
        stat_out[2, j : j + 1, :] = colsum[j, 1 - c][0:1]
        stat_out[3, j : j + 1, :] = colsum[PER + j, c][0:1]
    for k in range(3):
        send_stat(k).start()

    def start_second(j):
        send_far(1, j).start()

    loop(start_second)

    def finish_grad(j):
        send_part(PER + j).wait_recv()
        send_far(0, j).wait_recv()
        full = part[PER + j, c, 0:ROWS, :] + part_in[PER + j, 0:ROWS, :] + yr[j].astype(F32)
        gs[j] = full.astype(BF16)
        shift(0, j).start()

    loop(finish_grad)

    for k in range(3):
        send_stat(k).wait_recv()
    shares = [stat_in[0], stat_in[1], stat_in[2], stat_out[3]]
    tile = shares[0] + shares[1] + shares[2] + shares[3]
    mean_row = tile[3:4] / MODEL_WIDTH
    meansq = tile[4:5] / MODEL_WIDTH
    rstd_row = lax.rsqrt(meansq - mean_row * mean_row + EPS)
    mean = column(mean_row)
    rstd = column(rstd_row)
    offsets = [column(v[3:4] / DEPTH - mean_row) for v in shares]
    real = lengths[0]
    mask = (lax.broadcasted_iota(jnp.int32, (ROWS, HALF), 0) < real).astype(F32)
    mask_row = (lax.broadcasted_iota(jnp.int32, (1, HALF), 1) < real).astype(F32)

    first = jnp.zeros((ROWS, HALF), F32)
    second = jnp.zeros((ROWS, HALF), F32)
    for j in range(PER):
        send_far(1, j).wait_recv()
        full = (
            part[PER + j, c, ROWS : 2 * ROWS, :]
            + part_in[PER + j, ROWS : 2 * ROWS, :]
            + yr[PER + j].astype(F32)
        )
        for v, o in zip(shares, offsets):
            full = full + o * v[j : j + 1]
        z = rstd * full
        zs[j] = z
        ls[j] = (mask * z).astype(BF16)
        shift(1, j).start()
        shift(0, j).wait_recv()
        gather_far(0, j).start()
        gather_core(0, j).start()
    for j in range(PER):
        b = back[PER + j, c].astype(F32)
        first = first + b * tile[j : j + 1]
        second = second + b * zs[j]
    piece_out[...] = jnp.zeros(piece_out.shape, F32)
    piece_out[0:1, :] = row_of(first) * mask_row
    piece_out[1:2, :] = row_of(second) * mask_row
    for k in range(3):
        send_piece(k).start()

    def decode(acc, buf, p, fresh):
        left = jnp.concatenate([buf[p, 0], buf[p, 1]], axis=1)

        def step(n, carry):
            at = pl.ds(pl.multiple_of(n * CHUNK, CHUNK), CHUNK)
            d = lax.dot_general(
                left, enc[p, at, :], (((1,), (1,)), ((), ())), preferred_element_type=F32
            )
            acc[n] = acc[n] + d
            return carry

        lax.fori_loop(0, SPLIT, step, 0)

    acc_b[...] = jnp.zeros(acc_b.shape, F32)
    acc_r[...] = jnp.zeros(acc_r.shape, F32)

    def middle(j):
        shift(1, j).wait_recv()
        gather_far(1, j).start()
        gather_core(1, j).start()
        gather_core(0, j).wait_recv()
        decode(acc_b, back, PER + j, False)
        gather_far(0, j).wait_recv()
        pass_core(0, j).start()

    loop(middle)

    def late(j):
        pass_core(0, j).wait_recv()
        decode(acc_b, back, j, False)
        gather_core(1, j).wait_recv()
        decode(acc_r, recv, PER + j, False)
        gather_far(1, j).wait_recv()
        pass_core(1, j).start()

    loop(late)

    for k in range(3):
        send_piece(k).wait_recv()
    pieces = piece_out[...] + piece_in[0] + piece_in[1] + piece_in[2]
    first = column(pieces[0:1] / MODEL_WIDTH)
    second = column(pieces[1:2] / MODEL_WIDTH)

    def to_gradient(n):
        at = pl.ds(pl.multiple_of(n * CHUNK, CHUNK), CHUNK)
        return pltpu.make_async_copy(out_g.at[n], gradient.at[:, at], out_sem.at[n])

    def to_decoded(n):
        at = pl.ds(pl.multiple_of(n * CHUNK, CHUNK), CHUNK)
        return pltpu.make_async_copy(out_d.at[n], decoded.at[:, at], out_sem.at[SPLIT + n])

    for n in range(SPLIT):
        for i in range(CHUNK // HALF):
            lo = n * CHUNK + i * HALF
            v = x[ROWS : 2 * ROWS, lo : lo + HALF].astype(F32)
            normed = (v - mean) * rstd
            g = acc_b[n, :, i * HALF : (i + 1) * HALF] * mask
            out_g[n, :, i * HALF : (i + 1) * HALF] = (
                rstd * (g - first - normed * second)
            ).astype(BF16)
        to_gradient(n).start()

    def final(j):
        pass_core(1, j).wait_recv()
        decode(acc_r, recv, j, False)

    loop(final)
    for n in range(SPLIT):
        out_d[n] = acc_r[n].astype(BF16)
        to_decoded(n).start()

    def drain(p, carry):
        send_part(p).wait_send()
        return carry

    lax.fori_loop(0, BLOCKS, drain, 0)

    def drain_rest(j):
        for a in range(2):
            send_far(a, j).wait_send()
            shift(a, j).wait_send()
            gather_far(a, j).wait_send()
            gather_core(a, j).wait_send()
            pass_core(a, j).wait_send()

    loop(drain_rest)
    for k in range(3):
        send_stat(k).wait_send()
        send_piece(k).wait_send()
    for n in range(SPLIT):
        to_gradient(n).wait()
        to_decoded(n).wait()


def shards(sections, hidden, cotangent, encoder, lengths):
    any_space = pl.BlockSpec(memory_space=pl.ANY)
    sems = lambda n: pltpu.SemaphoreType.DMA((n,))
    return pl.pallas_call(
        functools.partial(kernel, sections),
        out_shape=(
            jax.ShapeDtypeStruct((ROWS, DEPTH), BF16),
            jax.ShapeDtypeStruct((ROWS, DEPTH), BF16),
        ),
        in_specs=[any_space, any_space, any_space, pl.BlockSpec(memory_space=pltpu.SMEM)],
        out_specs=(any_space, any_space),
        scratch_shapes=[
            pltpu.VMEM((2 * ROWS + 16, DEPTH), BF16),
            pltpu.VMEM((BLOCKS, DEPTH, BLOCK), BF16),
            pltpu.VMEM((BLOCKS, 2, 2 * ROWS, HALF), F32),
            pltpu.VMEM((BLOCKS, 2 * ROWS, HALF), F32),
            pltpu.VMEM((BLOCKS, 2, 8, HALF), F32),
            pltpu.VMEM((2 * PER, ROWS, HALF), BF16),
            pltpu.VMEM((2 * PER, ROWS, HALF), BF16),
            pltpu.VMEM((PER, ROWS, HALF), BF16),
            pltpu.VMEM((PER, ROWS, HALF), BF16),
            pltpu.VMEM((PER, ROWS, HALF), F32),
            pltpu.VMEM((BLOCKS, 2, ROWS, HALF), BF16),
            pltpu.VMEM((BLOCKS, 2, ROWS, HALF), BF16),
            pltpu.VMEM((4, 8, HALF), F32),
            pltpu.VMEM((3, 8, HALF), F32),
            pltpu.VMEM((8, HALF), F32),
            pltpu.VMEM((3, 8, HALF), F32),
            pltpu.VMEM((SPLIT, ROWS, CHUNK), F32),
            pltpu.VMEM((SPLIT, ROWS, CHUNK), F32),
            pltpu.VMEM((SPLIT, ROWS, CHUNK), BF16),
            pltpu.VMEM((SPLIT, ROWS, CHUNK), BF16),
            sems(2 + BLOCKS),
            sems(BLOCKS),
            sems(BLOCKS),
            sems(2 * PER),
            sems(2 * PER),
            sems(3),
            sems(3),
            sems(2 * PER),
            sems(2 * PER),
            sems(2 * PER),
            sems(2 * PER),
            sems(2 * PER),
            sems(2 * PER),
            sems(2 * PER),
            sems(2 * PER),
            sems(3),
            sems(3),
            sems(2 * SPLIT),
        ],
        compiler_params=pltpu.CompilerParams(
            collective_id=0, has_side_effects=True, vmem_limit_bytes=48 * 1024 * 1024
        ),
        name="relay",
    )(hidden, cotangent, encoder, lengths)


def solution(mesh):
    return jax.shard_map(
        functools.partial(shards, mesh.shape["section"]),
        mesh=mesh,
        in_specs=(P("section", "tensor"), P("section", "tensor"), P("tensor", None), P("section")),
        out_specs=(P("section", "tensor"), P("section", "tensor")),
        check_vma=False,
    )
```

```python
import functools

import jax
import jax.numpy as jnp
from jax import lax
from jax.experimental import pallas as pl
from jax.experimental.pallas import tpu as pltpu
from jax.sharding import PartitionSpec as P

MODEL_WIDTH = 12288
EPS = 1e-05
MESH = pl.DeviceIdType.MESH
F32 = jnp.float32
BF16 = jnp.bfloat16

ROWS = 128
DEPTH = 3072
BLOCK = 256
HALF = 128
PER = 3
BLOCKS = 2 * PER
SPLIT = 4
CHUNK = DEPTH // SPLIT


def column(row):
    return jnp.broadcast_to(row, (ROWS, HALF)).T


def row_of(square):
    return jnp.sum(square.T, axis=0, keepdims=True)


def kernel(
    sections,
    hidden,
    cotangent,
    encoder,
    lengths,
    decoded,
    gradient,
    x,
    enc,
    turned,
    part,
    part_in,
    colsum,
    ys,
    yr,
    gs,
    ls,
    zs,
    back,
    recv,
    stat_out,
    stat_in,
    piece_out,
    piece_in,
    acc_b,
    acc_r,
    load_sem,
    part_ss,
    part_rs,
    y_ss,
    y_rs,
    stat_ss,
    stat_rs,
    shift_ss,
    shift_rs,
    gy_ss,
    gy_rs,
    gd_ss,
    gd_rs,
    gf_ss,
    gf_rs,
    piece_ss,
    piece_rs,
):
    s = lax.axis_index("section")
    t = lax.axis_index("tensor")
    c = lax.rem(t, 2)
    chip = t // 2
    t_core = chip * 2 + (1 - c)
    t_far = (1 - chip) * 2 + c
    t_diag = (1 - chip) * 2 + (1 - c)
    core = {"section": s, "tensor": t_core}
    far = {"section": s, "tensor": t_far}
    diag = {"section": s, "tensor": t_diag}
    after = {"section": lax.rem(s + 1, sections), "tensor": t}
    before = {"section": lax.rem(s + sections - 1, sections), "tensor": t}
    peers = (core, far, diag)

    def remote(src, dst, ss, rs, to):
        return pltpu.make_async_remote_copy(
            src_ref=src, dst_ref=dst, send_sem=ss, recv_sem=rs, device_id=to, device_id_type=MESH
        )

    def load_encoder(p):
        b = lax.rem(PER * (1 - chip) + p, BLOCKS)
        at = pl.ds(pl.multiple_of(b * BLOCK, BLOCK), BLOCK)
        return pltpu.make_async_copy(encoder.at[:, at], enc.at[p], load_sem.at[2 + p])

    load_c = pltpu.make_async_copy(cotangent, x.at[pl.ds(0, ROWS)], load_sem.at[0])
    load_h = pltpu.make_async_copy(hidden, x.at[pl.ds(ROWS, ROWS)], load_sem.at[1])

    def send_part(p):
        return remote(part.at[p, 1 - c], part_in.at[p], part_ss.at[p], part_rs.at[p], core)

    def send_far(a, j):
        i = a * PER + j
        return remote(ys.at[i], yr.at[i], y_ss.at[i], y_rs.at[i], far)

    def send_stat(k):
        return remote(stat_out.at[k], stat_in.at[k], stat_ss.at[k], stat_rs.at[k], peers[k])

    def send_piece(k):
        return remote(piece_out, piece_in.at[k], piece_ss.at[k], piece_rs.at[k], peers[k])

    def shift(a, j):
        i = a * PER + j
        src, dst, to = ((gs, back, before), (ls, recv, after))[a]
        return remote(src.at[j], dst.at[PER + j, c], shift_ss.at[i], shift_rs.at[i], to)

    def gather_far(a, j):
        i = a * PER + j
        buf = (back, recv)[a]
        return remote(buf.at[PER + j, c], buf.at[j, c], gy_ss.at[i], gy_rs.at[i], far)

    def gather_core(a, j):
        i = a * PER + j
        buf = (back, recv)[a]
        return remote(buf.at[PER + j, c], buf.at[PER + j, c], gd_ss.at[i], gd_rs.at[i], core)

    def pass_core(a, j):
        i = a * PER + j
        buf = (back, recv)[a]
        return remote(buf.at[j, c], buf.at[j, c], gf_ss.at[i], gf_rs.at[i], core)

    def loop(body):
        def step(j, carry):
            body(j)
            return carry

        lax.fori_loop(0, PER, step, 0)

    load_h.start()
    load_c.start()
    load_encoder(0).start()
    load_encoder(1).start()
    barrier = pltpu.get_barrier_semaphore()
    for to in (core, far, diag, after, before):
        pl.semaphore_signal(barrier, inc=1, device_id=to, device_id_type=MESH)
    x[pl.ds(2 * ROWS, 16), :] = jnp.ones((16, DEPTH), BF16)

    load_h.wait()
    total = jnp.zeros((ROWS, HALF), F32)
    square = jnp.zeros((ROWS, HALF), F32)
    for i in range(DEPTH // HALF):
        v = x[ROWS : 2 * ROWS, i * HALF : (i + 1) * HALF].astype(F32)
        total = total + v
        square = square + v * v
    total = row_of(total)
    square = row_of(square)
    own_mean = total / DEPTH
    mean_here = column(own_mean)
    stat_out[...] = jnp.zeros(stat_out.shape, F32)
    for k in range(4):
        stat_out[k, 3:4, :] = total
        stat_out[k, 4:5, :] = square
    load_c.wait()

    def encode(p):
        load_encoder(p).wait()
        y = jnp.dot(x[...], enc[p], preferred_element_type=F32)
        for h in range(2):
            at = slice(h * HALF, (h + 1) * HALF)
            cs = y[2 * ROWS : 2 * ROWS + 1, at]
            part[p, h, 0:ROWS, :] = y[0:ROWS, at]
            part[p, h, ROWS : 2 * ROWS, :] = y[ROWS : 2 * ROWS, at] - mean_here * cs
            colsum[p, h] = y[2 * ROWS : 2 * ROWS + 8, at]

    def first_blocks(j):
        load_encoder(j + 2).start()
        encode(j)

    loop(first_blocks)
    load_encoder(PER + 2).start()
    pl.semaphore_wait(barrier, 5)

    def start_parts(j):
        send_part(j).start()

    loop(start_parts)

    def last_blocks(j):
        encode(PER + j)
        send_part(PER + j).start()
        send_part(j).wait_recv()
        total_here = part[j, c] + part_in[j]
        ys[j] = total_here[0:ROWS].astype(BF16)
        ys[PER + j] = total_here[ROWS : 2 * ROWS].astype(BF16)
        send_far(0, j).start()

    loop(last_blocks)

    for j in range(PER):
        stat_out[0, j : j + 1, :] = colsum[PER + j, 1 - c][0:1]
        stat_out[1, j : j + 1, :] = colsum[j, c][0:1]
        stat_out[2, j : j + 1, :] = colsum[j, 1 - c][0:1]
        stat_out[3, j : j + 1, :] = colsum[PER + j, c][0:1]
    for k in range(3):
        send_stat(k).start()

    def start_second(j):
        send_far(1, j).start()

    loop(start_second)

    def turn(p, carry):
        for n in range(SPLIT):
            turned[p, n] = enc[p, n * CHUNK : (n + 1) * CHUNK, :].T
        return carry

    acc_b[...] = jnp.zeros(acc_b.shape, F32)
    acc_r[...] = jnp.zeros(acc_r.shape, F32)
    lax.fori_loop(0, BLOCKS, turn, 0)

    def finish_grad(j):
        send_part(PER + j).wait_recv()
        send_far(0, j).wait_recv()
        full = part[PER + j, c, 0:ROWS, :] + part_in[PER + j, 0:ROWS, :] + yr[j].astype(F32)
        gs[j] = full.astype(BF16)
        shift(0, j).start()

    loop(finish_grad)

    for k in range(3):
        send_stat(k).wait_recv()
    shares = [stat_in[0], stat_in[1], stat_in[2], stat_out[3]]
    tile = shares[0] + shares[1] + shares[2] + shares[3]
    mean_row = tile[3:4] / MODEL_WIDTH
    meansq = tile[4:5] / MODEL_WIDTH
    rstd_row = lax.rsqrt(meansq - mean_row * mean_row + EPS)
    mean = column(mean_row)
    rstd = column(rstd_row)
    offsets = [column(v[3:4] / DEPTH - mean_row) for v in shares]
    real = lengths[0]
    mask = (lax.broadcasted_iota(jnp.int32, (ROWS, HALF), 0) < real).astype(F32)
    mask_row = (lax.broadcasted_iota(jnp.int32, (1, HALF), 1) < real).astype(F32)

    first = jnp.zeros((ROWS, HALF), F32)
    second = jnp.zeros((ROWS, HALF), F32)
    for j in range(PER):
        send_far(1, j).wait_recv()
        full = (
            part[PER + j, c, ROWS : 2 * ROWS, :]
            + part_in[PER + j, ROWS : 2 * ROWS, :]
            + yr[PER + j].astype(F32)
        )
        for v, o in zip(shares, offsets):
            full = full + o * v[j : j + 1]
        z = rstd * full
        zs[j] = z
        ls[j] = (mask * z).astype(BF16)
        shift(1, j).start()
        shift(0, j).wait_recv()
        gather_far(0, j).start()
        gather_core(0, j).start()
    for j in range(PER):
        b = back[PER + j, c].astype(F32)
        first = first + b * tile[j : j + 1]
        second = second + b * zs[j]
    piece_out[...] = jnp.zeros(piece_out.shape, F32)
    piece_out[0:1, :] = row_of(first) * mask_row
    piece_out[1:2, :] = row_of(second) * mask_row
    for k in range(3):
        send_piece(k).start()

    def decode(acc, buf, p):
        left = jnp.concatenate([buf[p, 0], buf[p, 1]], axis=1)

        def step(n, carry):
            acc[n] = acc[n] + jnp.dot(left, turned[p, n], preferred_element_type=F32)
            return carry

        lax.fori_loop(0, SPLIT, step, 0)

    def middle(j):
        shift(1, j).wait_recv()
        gather_far(1, j).start()
        gather_core(1, j).start()
        gather_core(0, j).wait_recv()
        decode(acc_b, back, PER + j)
        gather_far(0, j).wait_recv()
        pass_core(0, j).start()

    loop(middle)

    def late(j):
        pass_core(0, j).wait_recv()
        decode(acc_b, back, j)
        gather_core(1, j).wait_recv()
        decode(acc_r, recv, PER + j)
        gather_far(1, j).wait_recv()
        pass_core(1, j).start()

    loop(late)

    for k in range(3):
        send_piece(k).wait_recv()
    pieces = piece_out[...] + piece_in[0] + piece_in[1] + piece_in[2]
    first = column(pieces[0:1] / MODEL_WIDTH)
    second = column(pieces[1:2] / MODEL_WIDTH)

    for n in range(SPLIT):
        for i in range(CHUNK // HALF):
            lo = n * CHUNK + i * HALF
            v = x[ROWS : 2 * ROWS, lo : lo + HALF].astype(F32)
            normed = (v - mean) * rstd
            g = acc_b[n, :, i * HALF : (i + 1) * HALF] * mask
            gradient[:, lo : lo + HALF] = (rstd * (g - first - normed * second)).astype(BF16)

    def final(j):
        pass_core(1, j).wait_recv()
        decode(acc_r, recv, j)

    loop(final)
    for n in range(SPLIT):
        decoded[:, n * CHUNK : (n + 1) * CHUNK] = acc_r[n].astype(BF16)

    def drain(p, carry):
        send_part(p).wait_send()
        return carry

    lax.fori_loop(0, BLOCKS, drain, 0)

    def drain_rest(j):
        for a in range(2):
            send_far(a, j).wait_send()
            shift(a, j).wait_send()
            gather_far(a, j).wait_send()
            gather_core(a, j).wait_send()
            pass_core(a, j).wait_send()

    loop(drain_rest)
    for k in range(3):
        send_stat(k).wait_send()
        send_piece(k).wait_send()


def shards(sections, hidden, cotangent, encoder, lengths):
    hbm = pl.BlockSpec(memory_space=pltpu.HBM)
    vmem = pl.BlockSpec(memory_space=pltpu.VMEM)
    sems = lambda n: pltpu.SemaphoreType.DMA((n,))
    return pl.pallas_call(
        functools.partial(kernel, sections),
        out_shape=(
            jax.ShapeDtypeStruct((ROWS, DEPTH), BF16),
            jax.ShapeDtypeStruct((ROWS, DEPTH), BF16),
        ),
        in_specs=[hbm, hbm, hbm, pl.BlockSpec(memory_space=pltpu.SMEM)],
        out_specs=(vmem, vmem),
        scratch_shapes=[
            pltpu.VMEM((2 * ROWS + 16, DEPTH), BF16),
            pltpu.VMEM((BLOCKS, DEPTH, BLOCK), BF16),
            pltpu.VMEM((BLOCKS, SPLIT, BLOCK, CHUNK), BF16),
            pltpu.VMEM((BLOCKS, 2, 2 * ROWS, HALF), F32),
            pltpu.VMEM((BLOCKS, 2 * ROWS, HALF), F32),
            pltpu.VMEM((BLOCKS, 2, 8, HALF), F32),
            pltpu.VMEM((2 * PER, ROWS, HALF), BF16),
            pltpu.VMEM((2 * PER, ROWS, HALF), BF16),
            pltpu.VMEM((PER, ROWS, HALF), BF16),
            pltpu.VMEM((PER, ROWS, HALF), BF16),
            pltpu.VMEM((PER, ROWS, HALF), F32),
            pltpu.VMEM((BLOCKS, 2, ROWS, HALF), BF16),
            pltpu.VMEM((BLOCKS, 2, ROWS, HALF), BF16),
            pltpu.VMEM((4, 8, HALF), F32),
            pltpu.VMEM((3, 8, HALF), F32),
            pltpu.VMEM((8, HALF), F32),
            pltpu.VMEM((3, 8, HALF), F32),
            pltpu.VMEM((SPLIT, ROWS, CHUNK), F32),
            pltpu.VMEM((SPLIT, ROWS, CHUNK), F32),
            sems(2 + BLOCKS),
            sems(BLOCKS),
            sems(BLOCKS),
            sems(2 * PER),
            sems(2 * PER),
            sems(3),
            sems(3),
            sems(2 * PER),
            sems(2 * PER),
            sems(2 * PER),
            sems(2 * PER),
            sems(2 * PER),
            sems(2 * PER),
            sems(2 * PER),
            sems(2 * PER),
            sems(3),
            sems(3),
        ],
        compiler_params=pltpu.CompilerParams(
            collective_id=0, has_side_effects=True, vmem_limit_bytes=48 * 1024 * 1024
        ),
        name="relay",
    )(*[pltpu.with_memory_space_constraint(v, pltpu.HBM) for v in (hidden, cotangent, encoder)], lengths)


def solution(mesh):
    return jax.shard_map(
        functools.partial(shards, mesh.shape["section"]),
        mesh=mesh,
        in_specs=(P("section", "tensor"), P("section", "tensor"), P("tensor", None), P("section")),
        out_specs=(P("section", "tensor"), P("section", "tensor")),
        check_vma=False,
    )
```

```python
import functools

import jax
import jax.numpy as jnp
from jax import lax
from jax.experimental import pallas as pl
from jax.experimental.pallas import tpu as pltpu
from jax.sharding import PartitionSpec as P

MODEL_WIDTH = 12288
EPS = 1e-05
MESH = pl.DeviceIdType.MESH
F32 = jnp.float32
BF16 = jnp.bfloat16

ROWS = 128
DEPTH = 3072
BLOCK = 256
HALF = 128
PER = 3
BLOCKS = 2 * PER
SPLIT = 4
CHUNK = DEPTH // SPLIT


def column(row):
    return jnp.broadcast_to(row, (ROWS, HALF)).T


def row_of(square):
    return jnp.sum(square.T, axis=0, keepdims=True)


def kernel(
    sections,
    hidden,
    cotangent,
    encoder,
    lengths,
    decoded,
    gradient,
    x,
    enc,
    turned,
    part,
    part_in,
    colsum,
    ys,
    yr,
    gs,
    ls,
    zs,
    back,
    recv,
    stat_out,
    stat_in,
    piece_out,
    piece_in,
    acc_b,
    acc_r,
    load_sem,
    part_ss,
    part_rs,
    y_ss,
    y_rs,
    stat_ss,
    stat_rs,
    shift_ss,
    shift_rs,
    gy_ss,
    gy_rs,
    gd_ss,
    gd_rs,
    gf_ss,
    gf_rs,
    piece_ss,
    piece_rs,
):
    s = lax.axis_index("section")
    t = lax.axis_index("tensor")
    c = lax.rem(t, 2)
    chip = t // 2
    t_core = chip * 2 + (1 - c)
    t_far = (1 - chip) * 2 + c
    t_diag = (1 - chip) * 2 + (1 - c)
    core = {"section": s, "tensor": t_core}
    far = {"section": s, "tensor": t_far}
    diag = {"section": s, "tensor": t_diag}
    after = {"section": lax.rem(s + 1, sections), "tensor": t}
    before = {"section": lax.rem(s + sections - 1, sections), "tensor": t}
    peers = (core, far, diag)

    def remote(src, dst, ss, rs, to):
        return pltpu.make_async_remote_copy(
            src_ref=src, dst_ref=dst, send_sem=ss, recv_sem=rs, device_id=to, device_id_type=MESH
        )

    def load_encoder(p):
        b = lax.rem(PER * (1 - chip) + p, BLOCKS)
        at = pl.ds(pl.multiple_of(b * BLOCK, BLOCK), BLOCK)
        return pltpu.make_async_copy(encoder.at[:, at], enc.at[p], load_sem.at[2 + p])

    load_c = pltpu.make_async_copy(cotangent, x.at[pl.ds(0, ROWS)], load_sem.at[0])
    load_h = pltpu.make_async_copy(hidden, x.at[pl.ds(ROWS, ROWS)], load_sem.at[1])

    def send_part(p):
        return remote(part.at[p, 1 - c], part_in.at[p], part_ss.at[p], part_rs.at[p], core)

    def send_far(a, j):
        i = a * PER + j
        return remote(ys.at[i], yr.at[i], y_ss.at[i], y_rs.at[i], far)

    def send_stat(k):
        return remote(stat_out.at[k], stat_in.at[k], stat_ss.at[k], stat_rs.at[k], peers[k])

    def send_piece(k):
        return remote(piece_out, piece_in.at[k], piece_ss.at[k], piece_rs.at[k], peers[k])

    def shift(a, j):
        i = a * PER + j
        src, dst, to = ((gs, back, before), (ls, recv, after))[a]
        return remote(src.at[j], dst.at[PER + j, c], shift_ss.at[i], shift_rs.at[i], to)

    def gather_far(a, j):
        i = a * PER + j
        buf = (back, recv)[a]
        return remote(buf.at[PER + j, c], buf.at[j, c], gy_ss.at[i], gy_rs.at[i], far)

    def gather_core(a, j):
        i = a * PER + j
        buf = (back, recv)[a]
        return remote(buf.at[PER + j, c], buf.at[PER + j, c], gd_ss.at[i], gd_rs.at[i], core)

    def pass_core(a, j):
        i = a * PER + j
        buf = (back, recv)[a]
        return remote(buf.at[j, c], buf.at[j, c], gf_ss.at[i], gf_rs.at[i], core)

    def loop(body):
        def step(j, carry):
            body(j)
            return carry

        lax.fori_loop(0, PER, step, 0)

    load_h.start()
    load_c.start()
    load_encoder(0).start()
    load_encoder(1).start()
    barrier = pltpu.get_barrier_semaphore()
    for to in (core, far, diag, after, before):
        pl.semaphore_signal(barrier, inc=1, device_id=to, device_id_type=MESH)
    x[pl.ds(2 * ROWS, 16), :] = jnp.ones((16, DEPTH), BF16)

    load_h.wait()
    total = jnp.zeros((ROWS, HALF), F32)
    square = jnp.zeros((ROWS, HALF), F32)
    for i in range(DEPTH // HALF):
        v = x[ROWS : 2 * ROWS, i * HALF : (i + 1) * HALF].astype(F32)
        total = total + v
        square = square + v * v
    total = row_of(total)
    square = row_of(square)
    own_mean = total / DEPTH
    mean_here = column(own_mean)
    stat_out[...] = jnp.zeros(stat_out.shape, F32)
    for k in range(4):
        stat_out[k, 3:4, :] = total
        stat_out[k, 4:5, :] = square
    load_c.wait()

    def encode(p):
        load_encoder(p).wait()
        y = jnp.dot(x[...], enc[p], preferred_element_type=F32)
        for h in range(2):
            at = slice(h * HALF, (h + 1) * HALF)
            cs = y[2 * ROWS : 2 * ROWS + 1, at]
            part[p, h, 0:ROWS, :] = y[0:ROWS, at]
            part[p, h, ROWS : 2 * ROWS, :] = y[ROWS : 2 * ROWS, at] - mean_here * cs
            colsum[p, h] = y[2 * ROWS : 2 * ROWS + 8, at]

    def first_blocks(j):
        load_encoder(j + 2).start()
        encode(j)

    loop(first_blocks)
    load_encoder(PER + 2).start()
    pl.semaphore_wait(barrier, 5)

    def start_parts(j):
        send_part(j).start()

    loop(start_parts)

    def last_blocks(j):
        encode(PER + j)
        send_part(PER + j).start()
        send_part(j).wait_recv()
        total_here = part[j, c] + part_in[j]
        ys[j] = total_here[0:ROWS].astype(BF16)
        ys[PER + j] = total_here[ROWS : 2 * ROWS].astype(BF16)
        send_far(0, j).start()

    loop(last_blocks)

    for j in range(PER):
        stat_out[0, j : j + 1, :] = colsum[PER + j, 1 - c][0:1]
        stat_out[1, j : j + 1, :] = colsum[j, c][0:1]
        stat_out[2, j : j + 1, :] = colsum[j, 1 - c][0:1]
        stat_out[3, j : j + 1, :] = colsum[PER + j, c][0:1]
    for k in range(3):
        send_stat(k).start()

    def start_second(j):
        send_far(1, j).start()

    loop(start_second)

    def turn(p, carry):
        for n in range(SPLIT):
            turned[p, n] = enc[p, n * CHUNK : (n + 1) * CHUNK, :].T
        return carry

    acc_b[...] = jnp.zeros(acc_b.shape, F32)
    acc_r[...] = jnp.zeros(acc_r.shape, F32)
    lax.fori_loop(0, BLOCKS, turn, 0)

    def finish_grad(j):
        send_part(PER + j).wait_recv()
        send_far(0, j).wait_recv()
        full = part[PER + j, c, 0:ROWS, :] + part_in[PER + j, 0:ROWS, :] + yr[j].astype(F32)
        gs[j] = full.astype(BF16)
        shift(0, j).start()

    loop(finish_grad)

    for k in range(3):
        send_stat(k).wait_recv()
    shares = [stat_in[0], stat_in[1], stat_in[2], stat_out[3]]
    tile = shares[0] + shares[1] + shares[2] + shares[3]
    mean_row = tile[3:4] / MODEL_WIDTH
    meansq = tile[4:5] / MODEL_WIDTH
    rstd_row = lax.rsqrt(meansq - mean_row * mean_row + EPS)
    mean = column(mean_row)
    rstd = column(rstd_row)
    offsets = [column(v[3:4] / DEPTH - mean_row) for v in shares]
    real = lengths[0]
    mask = (lax.broadcasted_iota(jnp.int32, (ROWS, HALF), 0) < real).astype(F32)
    mask_row = (lax.broadcasted_iota(jnp.int32, (1, HALF), 1) < real).astype(F32)

    first = jnp.zeros((ROWS, HALF), F32)
    second = jnp.zeros((ROWS, HALF), F32)
    last = lax.rem(s, 12) == 11

    def start_back(j):
        shift(0, j).wait_recv()
        gather_far(0, j).start()
        gather_core(0, j).start()

    for j in range(PER):
        pl.when(jnp.logical_not(last))(functools.partial(start_back, j))
        send_far(1, j).wait_recv()
        full = (
            part[PER + j, c, ROWS : 2 * ROWS, :]
            + part_in[PER + j, ROWS : 2 * ROWS, :]
            + yr[PER + j].astype(F32)
        )
        for v, o in zip(shares, offsets):
            full = full + o * v[j : j + 1]
        z = rstd * full
        zs[j] = z
        ls[j] = (mask * z).astype(BF16)
        shift(1, j).start()
    for j in range(PER):
        pl.when(last)(functools.partial(start_back, j))
    for j in range(PER):
        b = back[PER + j, c].astype(F32)
        first = first + b * tile[j : j + 1]
        second = second + b * zs[j]
    piece_out[...] = jnp.zeros(piece_out.shape, F32)
    piece_out[0:1, :] = row_of(first) * mask_row
    piece_out[1:2, :] = row_of(second) * mask_row
    for k in range(3):
        send_piece(k).start()

    def decode(acc, buf, p):
        left = jnp.concatenate([buf[p, 0], buf[p, 1]], axis=1)

        def step(n, carry):
            acc[n] = acc[n] + jnp.dot(left, turned[p, n], preferred_element_type=F32)
            return carry

        lax.fori_loop(0, SPLIT, step, 0)

    for j in range(PER):
        shift(1, j).wait_recv()
        gather_far(1, j).start()
        gather_core(1, j).start()
        if j > 0:
            gather_far(0, j - 1).wait_recv()
            pass_core(0, j - 1).start()
        gather_core(0, j).wait_recv()
        decode(acc_b, back, PER + j)
    gather_far(0, PER - 1).wait_recv()
    pass_core(0, PER - 1).start()

    def late(j):
        pass_core(0, j).wait_recv()
        decode(acc_b, back, j)
        gather_core(1, j).wait_recv()
        decode(acc_r, recv, PER + j)

    loop(late)

    for k in range(3):
        send_piece(k).wait_recv()
    pieces = piece_out[...] + piece_in[0] + piece_in[1] + piece_in[2]
    first = column(pieces[0:1] / MODEL_WIDTH)
    second = column(pieces[1:2] / MODEL_WIDTH)

    for n in range(SPLIT):
        for i in range(CHUNK // HALF):
            lo = n * CHUNK + i * HALF
            v = x[ROWS : 2 * ROWS, lo : lo + HALF].astype(F32)
            normed = (v - mean) * rstd
            g = acc_b[n, :, i * HALF : (i + 1) * HALF] * mask
            gradient[:, lo : lo + HALF] = (rstd * (g - first - normed * second)).astype(BF16)

    for j in range(PER):
        gather_far(1, j).wait_recv()
        pass_core(1, j).start()
        if j > 0:
            pass_core(1, j - 1).wait_recv()
            decode(acc_r, recv, j - 1)
    pass_core(1, PER - 1).wait_recv()
    left = jnp.concatenate([recv[PER - 1, 0], recv[PER - 1, 1]], axis=1)
    for n in range(SPLIT):
        d = jnp.dot(left, turned[PER - 1, n], preferred_element_type=F32)
        decoded[:, n * CHUNK : (n + 1) * CHUNK] = (acc_r[n] + d).astype(BF16)

    def drain(p, carry):
        send_part(p).wait_send()
        return carry

    lax.fori_loop(0, BLOCKS, drain, 0)

    def drain_rest(j):
        for a in range(2):
            send_far(a, j).wait_send()
            shift(a, j).wait_send()
            gather_far(a, j).wait_send()
            gather_core(a, j).wait_send()
            pass_core(a, j).wait_send()

    loop(drain_rest)
    for k in range(3):
        send_stat(k).wait_send()
        send_piece(k).wait_send()


def shards(sections, hidden, cotangent, encoder, lengths):
    hbm = pl.BlockSpec(memory_space=pltpu.HBM)
    vmem = pl.BlockSpec(memory_space=pltpu.VMEM)
    sems = lambda n: pltpu.SemaphoreType.DMA((n,))
    return pl.pallas_call(
        functools.partial(kernel, sections),
        out_shape=(
            jax.ShapeDtypeStruct((ROWS, DEPTH), BF16),
            jax.ShapeDtypeStruct((ROWS, DEPTH), BF16),
        ),
        in_specs=[hbm, hbm, hbm, pl.BlockSpec(memory_space=pltpu.SMEM)],
        out_specs=(vmem, vmem),
        scratch_shapes=[
            pltpu.VMEM((2 * ROWS + 16, DEPTH), BF16),
            pltpu.VMEM((BLOCKS, DEPTH, BLOCK), BF16),
            pltpu.VMEM((BLOCKS, SPLIT, BLOCK, CHUNK), BF16),
            pltpu.VMEM((BLOCKS, 2, 2 * ROWS, HALF), F32),
            pltpu.VMEM((BLOCKS, 2 * ROWS, HALF), F32),
            pltpu.VMEM((BLOCKS, 2, 8, HALF), F32),
            pltpu.VMEM((2 * PER, ROWS, HALF), BF16),
            pltpu.VMEM((2 * PER, ROWS, HALF), BF16),
            pltpu.VMEM((PER, ROWS, HALF), BF16),
            pltpu.VMEM((PER, ROWS, HALF), BF16),
            pltpu.VMEM((PER, ROWS, HALF), F32),
            pltpu.VMEM((BLOCKS, 2, ROWS, HALF), BF16),
            pltpu.VMEM((BLOCKS, 2, ROWS, HALF), BF16),
            pltpu.VMEM((4, 8, HALF), F32),
            pltpu.VMEM((3, 8, HALF), F32),
            pltpu.VMEM((8, HALF), F32),
            pltpu.VMEM((3, 8, HALF), F32),
            pltpu.VMEM((SPLIT, ROWS, CHUNK), F32),
            pltpu.VMEM((SPLIT, ROWS, CHUNK), F32),
            sems(2 + BLOCKS),
            sems(BLOCKS),
            sems(BLOCKS),
            sems(2 * PER),
            sems(2 * PER),
            sems(3),
            sems(3),
            sems(2 * PER),
            sems(2 * PER),
            sems(2 * PER),
            sems(2 * PER),
            sems(2 * PER),
            sems(2 * PER),
            sems(2 * PER),
            sems(2 * PER),
            sems(3),
            sems(3),
        ],
        compiler_params=pltpu.CompilerParams(
            collective_id=0, has_side_effects=True, vmem_limit_bytes=48 * 1024 * 1024
        ),
        name="relay",
    )(*[pltpu.with_memory_space_constraint(v, pltpu.HBM) for v in (hidden, cotangent, encoder)], lengths)


def solution(mesh):
    return jax.shard_map(
        functools.partial(shards, mesh.shape["section"]),
        mesh=mesh,
        in_specs=(P("section", "tensor"), P("section", "tensor"), P("tensor", None), P("section")),
        out_specs=(P("section", "tensor"), P("section", "tensor")),
        check_vma=False,
    )
```

```python
import functools

import jax
import jax.numpy as jnp
from jax import lax
from jax.experimental import pallas as pl
from jax.experimental.pallas import tpu as pltpu
from jax.sharding import PartitionSpec as P

MODEL_WIDTH = 12288
EPS = 1e-05
MESH = pl.DeviceIdType.MESH
F32 = jnp.float32
BF16 = jnp.bfloat16

ROWS = 128
DEPTH = 3072
BLOCK = 256
HALF = 128
PER = 3
BLOCKS = 2 * PER
SPLIT = 4
CHUNK = DEPTH // SPLIT


def column(row):
    return jnp.broadcast_to(row, (ROWS, HALF)).T


def row_of(square):
    return jnp.sum(square.T, axis=0, keepdims=True)


def kernel(
    sections,
    hidden,
    cotangent,
    encoder,
    lengths,
    gradient,
    acc_r,
    left,
    turned_last,
    x,
    enc,
    turned,
    part,
    part_in,
    colsum,
    ys,
    yr,
    gs,
    ls,
    zs,
    back,
    recv,
    stat_out,
    stat_in,
    piece_out,
    piece_in,
    acc_b,
    load_sem,
    part_ss,
    part_rs,
    y_ss,
    y_rs,
    stat_ss,
    stat_rs,
    shift_ss,
    shift_rs,
    gy_ss,
    gy_rs,
    gd_ss,
    gd_rs,
    gf_ss,
    gf_rs,
    piece_ss,
    piece_rs,
):
    s = lax.axis_index("section")
    t = lax.axis_index("tensor")
    c = lax.rem(t, 2)
    chip = t // 2
    t_core = chip * 2 + (1 - c)
    t_far = (1 - chip) * 2 + c
    t_diag = (1 - chip) * 2 + (1 - c)
    core = {"section": s, "tensor": t_core}
    far = {"section": s, "tensor": t_far}
    diag = {"section": s, "tensor": t_diag}
    after = {"section": lax.rem(s + 1, sections), "tensor": t}
    before = {"section": lax.rem(s + sections - 1, sections), "tensor": t}
    peers = (core, far, diag)

    def remote(src, dst, ss, rs, to):
        return pltpu.make_async_remote_copy(
            src_ref=src, dst_ref=dst, send_sem=ss, recv_sem=rs, device_id=to, device_id_type=MESH
        )

    def load_encoder(p):
        b = lax.rem(PER * (1 - chip) + p, BLOCKS)
        at = pl.ds(pl.multiple_of(b * BLOCK, BLOCK), BLOCK)
        return pltpu.make_async_copy(encoder.at[:, at], enc.at[p], load_sem.at[2 + p])

    load_c = pltpu.make_async_copy(cotangent, x.at[pl.ds(0, ROWS)], load_sem.at[0])
    load_h = pltpu.make_async_copy(hidden, x.at[pl.ds(ROWS, ROWS)], load_sem.at[1])

    def send_part(p):
        return remote(part.at[p, 1 - c], part_in.at[p], part_ss.at[p], part_rs.at[p], core)

    def send_far(a, j):
        i = a * PER + j
        return remote(ys.at[i], yr.at[i], y_ss.at[i], y_rs.at[i], far)

    def send_stat(k):
        return remote(stat_out.at[k], stat_in.at[k], stat_ss.at[k], stat_rs.at[k], peers[k])

    def send_piece(k):
        return remote(piece_out, piece_in.at[k], piece_ss.at[k], piece_rs.at[k], peers[k])

    def shift(a, j):
        i = a * PER + j
        src, dst, to = ((gs, back, before), (ls, recv, after))[a]
        return remote(src.at[j], dst.at[PER + j, c], shift_ss.at[i], shift_rs.at[i], to)

    def gather_far(a, j):
        i = a * PER + j
        buf = (back, recv)[a]
        return remote(buf.at[PER + j, c], buf.at[j, c], gy_ss.at[i], gy_rs.at[i], far)

    def gather_core(a, j):
        i = a * PER + j
        buf = (back, recv)[a]
        return remote(buf.at[PER + j, c], buf.at[PER + j, c], gd_ss.at[i], gd_rs.at[i], core)

    def pass_core(a, j):
        i = a * PER + j
        buf = (back, recv)[a]
        return remote(buf.at[j, c], buf.at[j, c], gf_ss.at[i], gf_rs.at[i], core)

    def loop(body):
        def step(j, carry):
            body(j)
            return carry

        lax.fori_loop(0, PER, step, 0)

    load_h.start()
    load_c.start()
    load_encoder(0).start()
    load_encoder(1).start()
    barrier = pltpu.get_barrier_semaphore()
    for to in (core, far, diag, after, before):
        pl.semaphore_signal(barrier, inc=1, device_id=to, device_id_type=MESH)
    x[pl.ds(2 * ROWS, 16), :] = jnp.ones((16, DEPTH), BF16)

    load_h.wait()
    total = jnp.zeros((ROWS, HALF), F32)
    square = jnp.zeros((ROWS, HALF), F32)
    for i in range(DEPTH // HALF):
        v = x[ROWS : 2 * ROWS, i * HALF : (i + 1) * HALF].astype(F32)
        total = total + v
        square = square + v * v
    total = row_of(total)
    square = row_of(square)
    own_mean = total / DEPTH
    mean_here = column(own_mean)
    stat_out[...] = jnp.zeros(stat_out.shape, F32)
    for k in range(4):
        stat_out[k, 3:4, :] = total
        stat_out[k, 4:5, :] = square
    load_c.wait()

    def encode(p):
        load_encoder(p).wait()
        y = jnp.dot(x[...], enc[p], preferred_element_type=F32)
        for h in range(2):
            at = slice(h * HALF, (h + 1) * HALF)
            cs = y[2 * ROWS : 2 * ROWS + 1, at]
            part[p, h, 0:ROWS, :] = y[0:ROWS, at]
            part[p, h, ROWS : 2 * ROWS, :] = y[ROWS : 2 * ROWS, at] - mean_here * cs
            colsum[p, h] = y[2 * ROWS : 2 * ROWS + 8, at]

    def first_blocks(j):
        load_encoder(j + 2).start()
        encode(j)

    loop(first_blocks)
    load_encoder(PER + 2).start()
    pl.semaphore_wait(barrier, 5)

    def start_parts(j):
        send_part(j).start()

    loop(start_parts)

    def last_blocks(j):
        encode(PER + j)
        send_part(PER + j).start()
        send_part(j).wait_recv()
        total_here = part[j, c] + part_in[j]
        ys[j] = total_here[0:ROWS].astype(BF16)
        ys[PER + j] = total_here[ROWS : 2 * ROWS].astype(BF16)
        send_far(0, j).start()

    loop(last_blocks)

    for j in range(PER):
        stat_out[0, j : j + 1, :] = colsum[PER + j, 1 - c][0:1]
        stat_out[1, j : j + 1, :] = colsum[j, c][0:1]
        stat_out[2, j : j + 1, :] = colsum[j, 1 - c][0:1]
        stat_out[3, j : j + 1, :] = colsum[PER + j, c][0:1]
    for k in range(3):
        send_stat(k).start()

    def start_second(j):
        send_far(1, j).start()

    loop(start_second)

    def turn(p, carry):
        for n in range(SPLIT):
            turned[p, n] = enc[p, n * CHUNK : (n + 1) * CHUNK, :].T
        return carry

    acc_b[...] = jnp.zeros(acc_b.shape, F32)
    acc_r[...] = jnp.zeros(acc_r.shape, F32)
    lax.fori_loop(0, BLOCKS, turn, 0)
    for n in range(SPLIT):
        turned_last[n] = turned[PER - 1, n]

    def finish_grad(j):
        send_part(PER + j).wait_recv()
        send_far(0, j).wait_recv()
        full = part[PER + j, c, 0:ROWS, :] + part_in[PER + j, 0:ROWS, :] + yr[j].astype(F32)
        gs[j] = full.astype(BF16)
        shift(0, j).start()

    loop(finish_grad)

    for k in range(3):
        send_stat(k).wait_recv()
    shares = [stat_in[0], stat_in[1], stat_in[2], stat_out[3]]
    tile = shares[0] + shares[1] + shares[2] + shares[3]
    mean_row = tile[3:4] / MODEL_WIDTH
    meansq = tile[4:5] / MODEL_WIDTH
    rstd_row = lax.rsqrt(meansq - mean_row * mean_row + EPS)
    mean = column(mean_row)
    rstd = column(rstd_row)
    offsets = [column(v[3:4] / DEPTH - mean_row) for v in shares]
    real = lengths[0]
    mask = (lax.broadcasted_iota(jnp.int32, (ROWS, HALF), 0) < real).astype(F32)
    mask_row = (lax.broadcasted_iota(jnp.int32, (1, HALF), 1) < real).astype(F32)

    first = jnp.zeros((ROWS, HALF), F32)
    second = jnp.zeros((ROWS, HALF), F32)
    last = lax.rem(s, 12) == 11

    def start_back(j):
        shift(0, j).wait_recv()
        gather_far(0, j).start()
        gather_core(0, j).start()

    for j in range(PER):
        pl.when(jnp.logical_not(last))(functools.partial(start_back, j))
        send_far(1, j).wait_recv()
        full = (
            part[PER + j, c, ROWS : 2 * ROWS, :]
            + part_in[PER + j, ROWS : 2 * ROWS, :]
            + yr[PER + j].astype(F32)
        )
        for v, o in zip(shares, offsets):
            full = full + o * v[j : j + 1]
        z = rstd * full
        zs[j] = z
        ls[j] = (mask * z).astype(BF16)
        shift(1, j).start()
    for j in range(PER):
        pl.when(last)(functools.partial(start_back, j))
    for j in range(PER):
        b = back[PER + j, c].astype(F32)
        first = first + b * tile[j : j + 1]
        second = second + b * zs[j]
    piece_out[...] = jnp.zeros(piece_out.shape, F32)
    piece_out[0:1, :] = row_of(first) * mask_row
    piece_out[1:2, :] = row_of(second) * mask_row
    for k in range(3):
        send_piece(k).start()

    def decode(acc, buf, p):
        block = jnp.concatenate([buf[p, 0], buf[p, 1]], axis=1)

        def step(n, carry):
            acc[n] = acc[n] + jnp.dot(block, turned[p, n], preferred_element_type=F32)
            return carry

        lax.fori_loop(0, SPLIT, step, 0)

    for j in range(PER):
        shift(1, j).wait_recv()
        gather_far(1, j).start()
        gather_core(1, j).start()
        if j > 0:
            gather_far(0, j - 1).wait_recv()
            pass_core(0, j - 1).start()
        gather_core(0, j).wait_recv()
        decode(acc_b, back, PER + j)
    gather_far(0, PER - 1).wait_recv()
    pass_core(0, PER - 1).start()

    def late(j):
        pass_core(0, j).wait_recv()
        decode(acc_b, back, j)
        gather_core(1, j).wait_recv()
        decode(acc_r, recv, PER + j)

    loop(late)

    for k in range(3):
        send_piece(k).wait_recv()
    pieces = piece_out[...] + piece_in[0] + piece_in[1] + piece_in[2]
    first = column(pieces[0:1] / MODEL_WIDTH)
    second = column(pieces[1:2] / MODEL_WIDTH)

    for n in range(SPLIT):
        for i in range(CHUNK // HALF):
            lo = n * CHUNK + i * HALF
            v = x[ROWS : 2 * ROWS, lo : lo + HALF].astype(F32)
            normed = (v - mean) * rstd
            g = acc_b[n, :, i * HALF : (i + 1) * HALF] * mask
            gradient[:, lo : lo + HALF] = (rstd * (g - first - normed * second)).astype(BF16)

    for j in range(PER):
        gather_far(1, j).wait_recv()
        pass_core(1, j).start()
        if j > 0:
            pass_core(1, j - 1).wait_recv()
            decode(acc_r, recv, j - 1)
    pass_core(1, PER - 1).wait_recv()
    left[:, 0:HALF] = recv[PER - 1, 0]
    left[:, HALF:BLOCK] = recv[PER - 1, 1]

    def drain(p, carry):
        send_part(p).wait_send()
        return carry

    lax.fori_loop(0, BLOCKS, drain, 0)

    def drain_rest(j):
        for a in range(2):
            send_far(a, j).wait_send()
            shift(a, j).wait_send()
            gather_far(a, j).wait_send()
            gather_core(a, j).wait_send()
            pass_core(a, j).wait_send()

    loop(drain_rest)
    for k in range(3):
        send_stat(k).wait_send()
        send_piece(k).wait_send()


def finish_kernel(gradient, acc, left, turned_last, decoded_out, gradient_out, staged, sem):
    whole = pltpu.make_async_copy(gradient, gradient_out, sem.at[SPLIT])
    whole.start()
    copies = []
    for n in range(SPLIT):
        d = jnp.dot(left[...], turned_last[n], preferred_element_type=F32)
        staged[n] = (acc[n] + d).astype(BF16)
        at = pl.ds(n * CHUNK, CHUNK)
        copies.append(pltpu.make_async_copy(staged.at[n], decoded_out.at[:, at], sem.at[n]))
        copies[-1].start()
    for copy in copies:
        copy.wait()
    whole.wait()


def shards(sections, hidden, cotangent, encoder, lengths):
    hbm = pl.BlockSpec(memory_space=pltpu.HBM)
    vmem = pl.BlockSpec(memory_space=pltpu.VMEM)
    sems = lambda n: pltpu.SemaphoreType.DMA((n,))
    gradient, acc, left, turned_last = pl.pallas_call(
        functools.partial(kernel, sections),
        out_shape=(
            jax.ShapeDtypeStruct((ROWS, DEPTH), BF16),
            jax.ShapeDtypeStruct((SPLIT, ROWS, CHUNK), F32),
            jax.ShapeDtypeStruct((ROWS, BLOCK), BF16),
            jax.ShapeDtypeStruct((SPLIT, BLOCK, CHUNK), BF16),
        ),
        in_specs=[hbm, hbm, hbm, pl.BlockSpec(memory_space=pltpu.SMEM)],
        out_specs=(vmem,) * 4,
        scratch_shapes=[
            pltpu.VMEM((2 * ROWS + 16, DEPTH), BF16),
            pltpu.VMEM((BLOCKS, DEPTH, BLOCK), BF16),
            pltpu.VMEM((BLOCKS, SPLIT, BLOCK, CHUNK), BF16),
            pltpu.VMEM((BLOCKS, 2, 2 * ROWS, HALF), F32),
            pltpu.VMEM((BLOCKS, 2 * ROWS, HALF), F32),
            pltpu.VMEM((BLOCKS, 2, 8, HALF), F32),
            pltpu.VMEM((2 * PER, ROWS, HALF), BF16),
            pltpu.VMEM((2 * PER, ROWS, HALF), BF16),
            pltpu.VMEM((PER, ROWS, HALF), BF16),
            pltpu.VMEM((PER, ROWS, HALF), BF16),
            pltpu.VMEM((PER, ROWS, HALF), F32),
            pltpu.VMEM((BLOCKS, 2, ROWS, HALF), BF16),
            pltpu.VMEM((BLOCKS, 2, ROWS, HALF), BF16),
            pltpu.VMEM((4, 8, HALF), F32),
            pltpu.VMEM((3, 8, HALF), F32),
            pltpu.VMEM((8, HALF), F32),
            pltpu.VMEM((3, 8, HALF), F32),
            pltpu.VMEM((SPLIT, ROWS, CHUNK), F32),
            sems(2 + BLOCKS),
            sems(BLOCKS),
            sems(BLOCKS),
            sems(2 * PER),
            sems(2 * PER),
            sems(3),
            sems(3),
            sems(2 * PER),
            sems(2 * PER),
            sems(2 * PER),
            sems(2 * PER),
            sems(2 * PER),
            sems(2 * PER),
            sems(2 * PER),
            sems(2 * PER),
            sems(3),
            sems(3),
        ],
        compiler_params=pltpu.CompilerParams(
            collective_id=0, has_side_effects=True, vmem_limit_bytes=48 * 1024 * 1024
        ),
        name="relay",
    )(*[pltpu.with_memory_space_constraint(v, pltpu.HBM) for v in (hidden, cotangent, encoder)], lengths)
    return pl.pallas_call(
        finish_kernel,
        out_shape=(
            jax.ShapeDtypeStruct((ROWS, DEPTH), BF16),
            jax.ShapeDtypeStruct((ROWS, DEPTH), BF16),
        ),
        in_specs=[vmem] * 4,
        out_specs=(hbm, hbm),
        scratch_shapes=[
            pltpu.VMEM((SPLIT, ROWS, CHUNK), BF16),
            sems(SPLIT + 1),
        ],
        compiler_params=pltpu.CompilerParams(vmem_limit_bytes=16 * 1024 * 1024),
        name="finish",
    )(gradient, acc, left, turned_last)


def solution(mesh):
    return jax.shard_map(
        functools.partial(shards, mesh.shape["section"]),
        mesh=mesh,
        in_specs=(P("section", "tensor"), P("section", "tensor"), P("tensor", None), P("section")),
        out_specs=(P("section", "tensor"), P("section", "tensor")),
        check_vma=False,
    )
```
